32 devices in a mesh: row: 8 (over z, y), col: 4 (over x, core).
Axes of the slice: x: 2, y: 2, z: 4, core: 2. Of those that a mesh axis runs over, the one named last changes fastest.
Arguments:
- feat_one: bfloat16 [4096, 128], P(('row', 'col')), may hold values from -16 to 16
- feat_two: bfloat16 [4096, 128], P(('col', 'row')), may hold values from -16 to 16
- value_one: bfloat16 [4096, 128], P(('row', 'col')), may hold values from -6 to 6
- value_two: bfloat16 [4096, 128], P(('col', 'row')), may hold values from -6 to 6
Outputs:
- matched_one: float32 [4096, 128], P(('row', 'col'))
- flow_one: float32 [2, 4096], P(None, ('row', 'col'))
- matched_two: float32 [4096, 128], P(('col', 'row'))
- flow_two: float32 [2, 4096], P(None, ('col', 'row'))
The draws below stay inside these ranges and needn't reach their ends.
All inputs are finite; a program needn't handle non-finite values.
Results may differ from the reference program's by a relative error of at most 0.0011.
Values may be sent and summed in bfloat16 or wider, within the bound.
A program may use at most 128 MiB of HBM per device.

```python
import math
import jax
import jax.numpy as jnp
from jax import lax

FEAT = 128
GRID_W = 256
TOKENS = 4096
BLK = 512


def normal_features(key, salt):
    own = jax.random.fold_in(key, salt)
    key_noise, key_scale = jax.random.split(own)
    scales = jnp.exp(jax.random.uniform(key_scale, (TOKENS, 1), jnp.float32, math.log(0.8), math.log(3.0)))
    raw = jax.random.normal(key_noise, (TOKENS, FEAT), jnp.float32) * scales
    return jnp.clip(raw, -16.0, 16.0)


def draw_feat_one(key, part):
    raw = normal_features(key, 1103)
    return raw.astype(jnp.bfloat16)


def draw_feat_two(key, part):
    raw = normal_features(key, 2207)
    return raw.astype(jnp.bfloat16)


def levels(rng, shape, shards, smallest, largest):
    factor_of = 1.0
    for axis_at, blocks in shards:
        draws = jax.random.uniform(jax.random.fold_in(jax.random.fold_in(rng, 6), axis_at), (blocks,), jnp.float32, smallest / len(shards), largest / len(shards))
        factor_of = factor_of * jnp.repeat(jnp.exp(draws), shape[axis_at] // blocks).reshape((-1,) + (1,) * (len(shape) - 1 - axis_at))
    return factor_of


def gaussian(key, dims, spread, most, cuts=(), kind=jnp.bfloat16):
    drawn = spread * jax.random.normal(key, dims, jnp.float32)
    if cuts:
        drawn = drawn * levels(key, dims, cuts, -0.22, 0.18)
    return jnp.clip(drawn, -most, most).astype(kind)


def setup_inputs(seed: int = 0) -> dict:
    key_of = jax.random.split(jax.random.key(seed), 5)
    return {
        "feat_one": draw_feat_one(jax.random.fold_in(key_of[4], 71), 0),
        "feat_two": draw_feat_two(jax.random.fold_in(key_of[4], 71), 0),
        "value_one": gaussian(key_of[2], (TOKENS, FEAT), 1.0, 6.0, ((0, 32),)),
        "value_two": gaussian(key_of[3], (TOKENS, FEAT), 1.0, 6.0, ((0, 32),)),
    }


def token_coords(start, count, total):
    index = start + lax.iota(jnp.int32, count)
    across = (index % GRID_W).astype(jnp.float32) / GRID_W
    down = (index // GRID_W).astype(jnp.float32) / (total // GRID_W)
    return (across, down)

def flash_merge(first, second):
    peak_a, total_a, acc_a, across_a, down_a = first
    peak_b, total_b, acc_b, across_b, down_b = second
    peak = jnp.maximum(peak_a, peak_b)
    factor_a = jnp.exp(peak_a - peak)
    factor_b = jnp.exp(peak_b - peak)
    return (peak, total_a * factor_a + total_b * factor_b, acc_a * factor_a[:, None] + acc_b * factor_b[:, None], across_a * factor_a + across_b * factor_b, down_a * factor_a + down_b * factor_b)

def reference(feat_one, feat_two, value_one, value_two):
    scale = 1.0 / math.sqrt(FEAT)
    blocks = TOKENS // BLK
    all_across, all_down = token_coords(0, TOKENS, TOKENS)
    across_blocks = all_across.reshape(blocks, BLK)
    down_blocks = all_down.reshape(blocks, BLK)
    value_blocks = value_two.astype(jnp.float32).reshape(blocks, BLK, FEAT)

    def sweep(carry, block_index):
        start = (block_index * BLK).astype(jnp.int32)
        rows_feat = lax.dynamic_slice_in_dim(feat_one, start, BLK, 0)
        rows_value = lax.dynamic_slice_in_dim(value_one, start, BLK, 0)
        rows_across, rows_down = token_coords(start, BLK, TOKENS)
        scores = lax.dot_general(rows_feat, feat_two, (((1,), (1,)), ((), ())), preferred_element_type=jnp.float32) * scale
        tiled = scores.reshape(BLK, blocks, BLK)
        row_peak = lax.optimization_barrier(jnp.max(tiled, axis=2))
        row_weight = jnp.exp(tiled - row_peak[:, :, None]).astype(jnp.bfloat16)
        weight_f = row_weight.astype(jnp.float32)
        part_total = lax.optimization_barrier(jnp.sum(weight_f, axis=2))
        part_across = lax.optimization_barrier(jnp.sum(weight_f * across_blocks[None], axis=2))
        part_down = lax.optimization_barrier(jnp.sum(weight_f * down_blocks[None], axis=2))
        part_acc = jnp.einsum('rkt,ktc->rkc', weight_f, value_blocks)
        row_top = lax.optimization_barrier(jnp.max(row_peak, axis=1))
        factor = jnp.exp(row_peak - row_top[:, None])
        row_out = (row_top, lax.optimization_barrier(jnp.sum(factor * part_total, axis=1)), lax.optimization_barrier(jnp.sum(factor[:, :, None] * part_acc, axis=1)), lax.optimization_barrier(jnp.sum(factor * part_across, axis=1)), lax.optimization_barrier(jnp.sum(factor * part_down, axis=1)))
        col_peak = lax.optimization_barrier(jnp.max(scores, axis=0))
        col_weight = jnp.exp(scores - col_peak[None]).astype(jnp.bfloat16)
        cweight_f = col_weight.astype(jnp.float32)
        col_acc = jnp.dot(cweight_f.T, rows_value.astype(jnp.float32), precision=lax.Precision.HIGHEST)
        col_part = (col_peak, lax.optimization_barrier(jnp.sum(cweight_f, axis=0)), col_acc, lax.optimization_barrier(jnp.sum(cweight_f * rows_across[:, None], axis=0)), lax.optimization_barrier(jnp.sum(cweight_f * rows_down[:, None], axis=0)))
        return (flash_merge(carry, col_part), row_out)
    init = (jnp.full((TOKENS,), -jnp.inf, jnp.float32), jnp.zeros((TOKENS,), jnp.float32), jnp.zeros((TOKENS, FEAT), jnp.float32), jnp.zeros((TOKENS,), jnp.float32), jnp.zeros((TOKENS,), jnp.float32))
    carry, row_out = lax.scan(sweep, init, jnp.arange(blocks, dtype=jnp.int32))
    row_total = row_out[1].reshape(TOKENS)
    row_acc = row_out[2].reshape(TOKENS, FEAT)
    row_across = row_out[3].reshape(TOKENS)
    row_down = row_out[4].reshape(TOKENS)
    matched_one = row_acc / row_total[:, None]
    flow_one = jnp.stack([row_across / row_total - all_across, row_down / row_total - all_down])
    col_total, col_acc, col_across, col_down = (carry[1], carry[2], carry[3], carry[4])
    matched_two = col_acc / col_total[:, None]
    flow_two = jnp.stack([col_across / col_total - all_across, col_down / col_total - all_down])
    return (matched_one, flow_one, matched_two, flow_two)
```

```python
import functools
import math

import jax
import jax.numpy as jnp
from jax import lax
from jax.experimental import pallas as pl
from jax.experimental.pallas import tpu as pltpu
from jax.sharding import PartitionSpec as P

GRID_W = 256
EXTRA = 16
STATS = 8
MESH = pl.DeviceIdType.MESH


def split_axes(rows, cols):
    cores = 2 if cols % 2 == 0 else 1
    outer = cols // cores
    low = min(
        (n for n in range(1, rows + 1) if rows % n == 0),
        key=lambda n: abs(n * outer - rows // n),
    )
    return rows // low, low, outer, cores


def coords(block, shard, total, shape):
    index = block * shard + lax.broadcasted_iota(jnp.int32, shape, len(shape) - 1)
    across = lax.rem(index, GRID_W).astype(jnp.float32) / GRID_W
    down = lax.div(index, GRID_W).astype(jnp.float32) / (total // GRID_W)
    return across, down


def values_under(block, value, shard, total):
    across, down = coords(block, shard, total, (EXTRA, shard))
    line = lax.broadcasted_iota(jnp.int32, (EXTRA, shard), 0)
    extra = jnp.where(line == 0, 1.0, jnp.where(line == 1, across, jnp.where(line == 2, down, 0.0)))
    turned = jnp.transpose(value.astype(jnp.float32))
    return jnp.concatenate([turned, extra], axis=0).astype(jnp.bfloat16)


def attend(keys, queries, under, width, rate):
    scores = lax.dot_general(
        keys, queries, (((1,), (1,)), ((), ())), preferred_element_type=jnp.float32
    )
    peak = jnp.max(scores, axis=0, keepdims=True)
    weight = jnp.exp2((scores - peak) * rate).astype(jnp.bfloat16)
    sums = jnp.dot(under, weight, preferred_element_type=jnp.float32)
    stats = sums[width : width + STATS]
    line = lax.broadcasted_iota(jnp.int32, stats.shape, 0)
    stats = jnp.where(line == 3, peak, stats)
    return jnp.concatenate([sums[:width], stats], axis=0)


def merge(packets, width, rate):
    peaks = [p[width + 3 : width + 4] for p in packets]
    top = functools.reduce(jnp.maximum, peaks)
    total = None
    for packet, peak in zip(packets, peaks):
        term = packet * jnp.exp2((peak - top) * rate)
        total = term if total is None else total + term
    return total, top


def kernel(
    dims, total, rate,
    feat_one, feat_two, value_one, value_two,
    matched_one, flow_one, matched_two, flow_two,
    f1, v1, f2, v2, under1, under2, part1, pair1, send1, got1, part2, got2,
    load_sem, f1s, f1r, v1s, v1r, g1s, g1r, w1s, w1r, f2s, f2r, v2s, v2r,
    p2s, p2r, q1s, q1r, p1s, p1r,
):
    high, low, outer, cores = dims
    rows, cols = high * low, outer * cores
    plane = low * outer
    shard, width = feat_one.shape
    row, col = lax.axis_index("row"), lax.axis_index("col")
    h, l = row // low, row % low
    x, k = col // cores, col % cores
    p = l * outer + x

    def in_plane(step):
        q = (p + step + plane) % plane
        return (h * low + q // outer, (q % outer) * cores + k)

    def in_line(step):
        return (((h + step + high) % high) * low + l, col)

    partner = (row, x * cores + (cores - 1 - k))

    def block_one(slot):
        q = (p - slot % plane + plane) % plane
        core = k if slot < plane else cores - 1 - k
        return (h * low + q // outer) * cols + (q % outer) * cores + core

    def block_two(slot):
        return col * rows + ((h - slot + high) % high) * low + l

    def span(slot):
        return pl.ds(slot * shard, shard)

    loads = [
        pltpu.make_async_copy(src, dst.at[span(0)], load_sem.at[n])
        for n, (src, dst) in enumerate(
            ((feat_two, f2), (feat_one, f1), (value_one, v1), (value_two, v2))
        )
    ]
    for load in loads:
        load.start()

    peers = [in_plane(d) for d in range(1, plane)] + [in_line(e) for e in range(1, high)]
    if cores == 2:
        peers.append(partner)
    barrier = pltpu.get_barrier_semaphore()
    for peer in peers:
        pl.semaphore_signal(barrier, inc=1, device_id=peer, device_id_type=MESH)
    pl.semaphore_wait(barrier, len(peers))

    started = []

    def send(src, dst, ssem, rsem, peer):
        copy = pltpu.make_async_remote_copy(
            src_ref=src, dst_ref=dst, send_sem=ssem, recv_sem=rsem,
            device_id=peer, device_id_type=MESH,
        )
        copy.start()
        started.append(copy)
        return copy

    def gather(buf, ssem, rsem, count, peer_of):
        return [None] + [
            send(buf.at[span(0)], buf.at[span(s)], ssem.at[s], rsem.at[s], peer_of(s))
            for s in range(1, count)
        ]

    def forward(buf, slot, ssem, rsem):
        return send(
            buf.at[span(slot)], buf.at[span(plane + slot)], ssem.at[slot], rsem.at[slot], partner
        )

    loads[0].wait()
    f2c = gather(f2, f2s, f2r, high, in_line)
    loads[1].wait()
    f1c = gather(f1, f1s, f1r, plane, in_plane)
    loads[2].wait()
    v1c = gather(v1, v1s, v1r, plane, in_plane)
    loads[3].wait()
    v2c = gather(v2, v2s, v2r, high, in_line)
    f1f, v1f = [], []

    def keep_one(slot):
        under1[:, span(slot)] = values_under(block_one(slot), v1[span(slot), :], shard, total)

    for s in range(plane):
        if s:
            f1c[s].wait_recv()
        if cores == 2:
            f1f.append(forward(f1, s, g1s, g1r))
        if s:
            v1c[s].wait_recv()
        if cores == 2:
            v1f.append(forward(v1, s, w1s, w1r))
        keep_one(s)
    if cores == 2:
        for s in range(plane):
            f1f[s].wait_recv()
            v1f[s].wait_recv()
            keep_one(plane + s)

    p2c = []
    for s in range(high):
        if s:
            f2c[s].wait_recv()
        part2[s] = attend(f1[...], f2[span(s), :], under1[...], width, rate)
        if s:
            p2c.append(send(part2.at[s], got2.at[s], p2s.at[s], p2r.at[s], in_line(-s)))
    for s in range(high):
        if s:
            v2c[s].wait_recv()
        under2[:, span(s)] = values_under(block_two(s), v2[span(s), :], shard, total)

    step = 2 if plane % 2 == 0 else 1
    q1c, p1c = [], []
    for kind in reversed(range(cores)):
        for s in range(0, plane, step):
            first = kind * plane + s
            out = attend(
                f2[...], f1[pl.ds(first * shard, step * shard), :], under2[...], width, rate
            )
            for n in range(step):
                part1[first + n] = out[:, n * shard : (n + 1) * shard]
                if kind == 1:
                    q1c.append(
                        send(part1.at[first + n], pair1.at[s + n], q1s.at[s + n], q1r.at[s + n], partner)
                    )
    line = lax.broadcasted_iota(jnp.int32, (width + STATS, shard), 0)
    for s in reversed(range(plane)):
        if cores == 2:
            q1c[s].wait_recv()
            sums, top = merge([part1[s], pair1[s]], width, rate)
            send1[s] = jnp.where(line == width + 3, top, sums)
        else:
            send1[s] = part1[s]
        if s:
            p1c.append(send(send1.at[s], got1.at[s], p1s.at[s], p1r.at[s], in_plane(-s)))

    def finish(packets, block, matched, flow):
        sums, _ = merge(packets, width, rate)
        inverse = 1.0 / sums[width : width + 1]
        matched[...] = jnp.transpose(sums[:width] * inverse)
        across, down = coords(block, shard, total, (1, shard))
        flow[0:1, :] = sums[width + 1 : width + 2] * inverse - across
        flow[1:2, :] = sums[width + 2 : width + 3] * inverse - down

    for copy in p2c:
        copy.wait_recv()
    finish([part2[0]] + [got2[s] for s in range(1, high)], block_two(0), matched_two, flow_two)
    for copy in p1c:
        copy.wait_recv()
    finish([send1[0]] + [got1[s] for s in range(1, plane)], block_one(0), matched_one, flow_one)
    for copy in started:
        copy.wait_send()


def body(feat_one, feat_two, value_one, value_two):
    shard, width = feat_one.shape
    rows, cols = lax.axis_size("row"), lax.axis_size("col")
    dims = split_axes(rows, cols)
    high, low, outer, cores = dims
    plane = low * outer
    total = shard * rows * cols
    rate = math.log2(math.e) / math.sqrt(width)
    bf16, f32 = jnp.bfloat16, jnp.float32
    n1, n2 = plane * cores * shard, high * shard
    packet = (width + STATS, shard)
    vmem = pltpu.VMEM
    dma = pltpu.SemaphoreType.DMA
    return pl.pallas_call(
        functools.partial(kernel, dims, total, rate),
        out_shape=(
            jax.ShapeDtypeStruct((shard, width), f32),
            jax.ShapeDtypeStruct((2, shard), f32),
            jax.ShapeDtypeStruct((shard, width), f32),
            jax.ShapeDtypeStruct((2, shard), f32),
        ),
        in_specs=[pl.BlockSpec(memory_space=pl.ANY)] * 4,
        out_specs=[pl.BlockSpec(memory_space=pltpu.VMEM)] * 4,
        scratch_shapes=[
            vmem((n1, width), bf16),
            vmem((n1, width), bf16),
            vmem((n2, width), bf16),
            vmem((n2, width), bf16),
            vmem((width + EXTRA, n1), bf16),
            vmem((width + EXTRA, n2), bf16),
            vmem((plane * cores,) + packet, f32),
            vmem((plane,) + packet, f32),
            vmem((plane,) + packet, f32),
            vmem((plane,) + packet, f32),
            vmem((high,) + packet, f32),
            vmem((high,) + packet, f32),
            dma((4,)),
        ]
        + [dma((plane,))] * 8
        + [dma((high,))] * 6
        + [dma((plane,))] * 4,
        compiler_params=pltpu.CompilerParams(collective_id=0, has_side_effects=True),
        name="match",
    )(feat_one, feat_two, value_one, value_two)


def solution(mesh):
    return jax.shard_map(
        body,
        mesh=mesh,
        in_specs=(
            P(("row", "col"), None),
            P(("col", "row"), None),
            P(("row", "col"), None),
            P(("col", "row"), None),
        ),
        out_specs=(
            P(("row", "col"), None),
            P(None, ("row", "col")),
            P(("col", "row"), None),
            P(None, ("col", "row")),
        ),
        check_vma=False,
    )
```

```python
import functools
import math

import jax
import jax.numpy as jnp
from jax import lax
from jax.experimental import pallas as pl
from jax.experimental.pallas import tpu as pltpu
from jax.sharding import PartitionSpec as P

GRID_W = 256
EXTRA = 16
STATS = 8
SPAN = 240.0
MESH = pl.DeviceIdType.MESH


def split_axes(rows, cols):
    cores = 2 if cols % 2 == 0 else 1
    outer = cols // cores
    low = min(
        (n for n in range(1, rows + 1) if rows % n == 0),
        key=lambda n: abs(n * outer - rows // n),
    )
    return rows // low, low, outer, cores


def coords(block, shard, total, shape):
    index = block * shard + lax.broadcasted_iota(jnp.int32, shape, len(shape) - 1)
    across = lax.rem(index, GRID_W).astype(jnp.float32) / GRID_W
    down = lax.div(index, GRID_W).astype(jnp.float32) / (total // GRID_W)
    return across, down


def values_under(block, value, shard, total):
    across, down = coords(block, shard, total, (EXTRA, shard))
    line = lax.broadcasted_iota(jnp.int32, (EXTRA, shard), 0)
    extra = jnp.where(line == 0, 1.0, jnp.where(line == 1, across, jnp.where(line == 2, down, 0.0)))
    turned = jnp.transpose(value.astype(jnp.float32))
    return jnp.concatenate([turned, extra], axis=0).astype(jnp.bfloat16)


def weigh(keys, queries, rate):
    scores = lax.dot_general(
        keys, queries, (((1,), (1,)), ((), ())), preferred_element_type=jnp.float32
    )
    peak = jnp.max(scores, axis=0, keepdims=True)
    return jnp.exp2((scores - peak) * rate).astype(jnp.bfloat16), peak


def collect(under, weight, peak, width):
    sums = jnp.dot(under, weight, preferred_element_type=jnp.float32)
    acc, stats = sums[:width], sums[width : width + STATS]
    line = lax.broadcasted_iota(jnp.int32, stats.shape, 0)
    return acc, jnp.where(line == 3, peak, stats)


def encode(acc, stats):
    size = jnp.abs(acc)
    big = jnp.maximum(jnp.max(size, axis=0, keepdims=True), 1e-30)
    code = jnp.exp2(size * (SPAN / big) - SPAN / 2)
    line = lax.broadcasted_iota(jnp.int32, stats.shape, 0)
    return jnp.where(acc < 0, -code, code).astype(jnp.bfloat16), jnp.where(line == 4, big, stats)


def decode(code, stats):
    code = code.astype(jnp.float32)
    size = jnp.log(jnp.abs(code)) * (1.0 / (SPAN * math.log(2.0))) + 0.5
    return jnp.where(code < 0, -size, size) * stats[4:5]


def merge(packets, rate):
    top = functools.reduce(jnp.maximum, [stats[3:4] for _, stats in packets])
    acc_all, stats_all = 0.0, 0.0
    for acc, stats in packets:
        factor = jnp.exp2((stats[3:4] - top) * rate)
        acc_all += acc * factor
        stats_all += stats * factor
    return acc_all, stats_all


def kernel(
    dims, total, rate,
    feat_one, feat_two, value_one, value_two,
    out_one, out_two,
    f1, v1, f2, v2, under1, under2, weight1, peak1, own1, own2,
    code1, stat1, got_code1, got_stat1, code2, stat2, got_code2, got_stat2,
    load_sem, f1s, f1r, v1s, v1r, g1s, g1r, w1s, w1r, f2s, f2r, v2s, v2r,
    c2s, c2r, t2s, t2r, c1s, c1r, t1s, t1r,
):
    high, low, outer, cores = dims
    rows, cols = high * low, outer * cores
    plane = low * outer
    shard, width = feat_one.shape
    row, col = lax.axis_index("row"), lax.axis_index("col")
    h, l = row // low, row % low
    x, k = col // cores, col % cores
    p = l * outer + x

    def in_plane(step, kind=0):
        q = (p + step + plane) % plane
        return (h * low + q // outer, (q % outer) * cores + (cores - 1 - k if kind else k))

    def in_line(step):
        return (((h + step + high) % high) * low + l, col)

    partner = in_plane(0, 1)

    def block_one(slot):
        q = (p - slot % plane + plane) % plane
        core = k if slot < plane else cores - 1 - k
        return (h * low + q // outer) * cols + (q % outer) * cores + core

    def block_two(slot):
        return col * rows + ((h - slot + high) % high) * low + l

    def span(slot):
        return pl.ds(slot * shard, shard)

    loads = [
        pltpu.make_async_copy(src, dst.at[span(0)], load_sem.at[n])
        for n, (src, dst) in enumerate(
            ((feat_two, f2), (feat_one, f1), (value_one, v1), (value_two, v2))
        )
    ]
    for load in loads:
        load.start()

    peers = [in_line(e) for e in range(1, high)]
    peers += [in_plane(d, kind) for kind in range(cores) for d in range(plane) if d or kind]
    barrier = pltpu.get_barrier_semaphore()
    for peer in peers:
        pl.semaphore_signal(barrier, inc=1, device_id=peer, device_id_type=MESH)
    pl.semaphore_wait(barrier, len(peers))

    started = []

    def send(src, dst, ssem, rsem, peer):
        copy = pltpu.make_async_remote_copy(
            src_ref=src, dst_ref=dst, send_sem=ssem, recv_sem=rsem,
            device_id=peer, device_id_type=MESH,
        )
        copy.start()
        started.append(copy)
        return copy

    def gather(buf, ssem, rsem, count, peer_of):
        return [None] + [
            send(buf.at[span(0)], buf.at[span(s)], ssem.at[s], rsem.at[s], peer_of(s))
            for s in range(1, count)
        ]

    def forward(buf, slot, ssem, rsem):
        return send(
            buf.at[span(slot)], buf.at[span(plane + slot)], ssem.at[slot], rsem.at[slot], partner
        )

    loads[0].wait()
    f2c = gather(f2, f2s, f2r, high, in_line)
    loads[1].wait()
    f1c = gather(f1, f1s, f1r, plane, in_plane)
    loads[2].wait()
    v1c = gather(v1, v1s, v1r, plane, in_plane)
    loads[3].wait()
    v2c = gather(v2, v2s, v2r, high, in_line)
    f1f, v1f = [], []

    def keep_one(slot):
        under1[:, span(slot)] = values_under(block_one(slot), v1[span(slot), :], shard, total)

    for s in range(plane):
        if s:
            f1c[s].wait_recv()
        if cores == 2:
            f1f.append(forward(f1, s, g1s, g1r))
    for s in range(plane):
        if s:
            v1c[s].wait_recv()
        if cores == 2:
            v1f.append(forward(v1, s, w1s, w1r))
        keep_one(s)
    if cores == 2:
        for s in range(plane):
            f1f[s].wait_recv()
            v1f[s].wait_recv()
            keep_one(plane + s)

    c2c, c1c = [], []
    for s in range(high):
        if s:
            f2c[s].wait_recv()
        acc, stats = collect(under1[...], *weigh(f1[...], f2[span(s), :], rate), width)
        if s:
            code2[s], stat2[s] = encode(acc, stats)
            c2c.append(send(code2.at[s], got_code2.at[s], c2s.at[s], c2r.at[s], in_line(-s)))
            c2c.append(send(stat2.at[s], got_stat2.at[s], t2s.at[s], t2r.at[s], in_line(-s)))
        else:
            own2[:width], own2[width:] = acc, stats

    step = 2 if plane % 2 == 0 else 1
    for s in range(0, plane * cores, step):
        at = pl.ds(s * shard, step * shard)
        weight1[:, at], peak1[:, at] = weigh(f2[...], f1[at, :], rate)
    for s in range(high):
        if s:
            v2c[s].wait_recv()
        under2[:, span(s)] = values_under(block_two(s), v2[span(s), :], shard, total)
    for s in reversed(range(0, plane * cores, step)):
        at = pl.ds(s * shard, step * shard)
        accs, statss = collect(under2[...], weight1[:, at], peak1[:, at], width)
        for n in range(step):
            slot, lanes = s + n, slice(n * shard, (n + 1) * shard)
            acc, stats = accs[:, lanes], statss[:, lanes]
            if slot:
                owner = in_plane(-(slot % plane), slot // plane)
                code1[slot], stat1[slot] = encode(acc, stats)
                c1c.append(
                    send(code1.at[slot], got_code1.at[slot], c1s.at[slot], c1r.at[slot], owner)
                )
                c1c.append(
                    send(stat1.at[slot], got_stat1.at[slot], t1s.at[slot], t1r.at[slot], owner)
                )
            else:
                own1[:width], own1[width:] = acc, stats

    def finish(own, codes, stats, count, block, out):
        packets = [(own[:width], own[width:])]
        packets += [(decode(codes[n], stats[n]), stats[n]) for n in range(1, count)]
        acc, sums = merge(packets, rate)
        inverse = 1.0 / sums[0:1]
        out[:width] = acc * inverse
        across, down = coords(block, shard, total, (STATS, shard))
        line = lax.broadcasted_iota(jnp.int32, sums.shape, 0)
        out[width:] = sums * inverse - jnp.where(line == 1, across, down)

    for copy in c2c:
        copy.wait_recv()
    finish(own2, got_code2, got_stat2, high, block_two(0), out_two)
    for copy in c1c:
        copy.wait_recv()
    finish(own1, got_code1, got_stat1, plane * cores, block_one(0), out_one)
    for copy in started:
        copy.wait_send()


def place(one, two, matched_one, flow_one, matched_two, flow_two):
    width = matched_one.shape[1]
    for packet, matched, flow in ((one, matched_one, flow_one), (two, matched_two, flow_two)):
        matched[...] = jnp.transpose(packet[:width])
        flow[...] = packet[width + 1 : width + 3]


def body(feat_one, feat_two, value_one, value_two):
    shard, width = feat_one.shape
    rows, cols = lax.axis_size("row"), lax.axis_size("col")
    dims = split_axes(rows, cols)
    high, low, outer, cores = dims
    plane = low * outer
    total = shard * rows * cols
    rate = math.log2(math.e) / math.sqrt(width)
    bf16, f32 = jnp.bfloat16, jnp.float32
    n1, n2 = plane * cores * shard, high * shard
    packet = (width + STATS, shard)
    vmem = pltpu.VMEM
    dma = pltpu.SemaphoreType.DMA
    one, two = pl.pallas_call(
        functools.partial(kernel, dims, total, rate),
        out_shape=(jax.ShapeDtypeStruct(packet, f32),) * 2,
        in_specs=[pl.BlockSpec(memory_space=pltpu.HBM)] * 4,
        out_specs=[pl.BlockSpec(memory_space=pltpu.VMEM)] * 2,
        scratch_shapes=[
            vmem((n1, width), bf16),
            vmem((n1, width), bf16),
            vmem((n2, width), bf16),
            vmem((n2, width), bf16),
            vmem((width + EXTRA, n1), bf16),
            vmem((width + EXTRA, n2), bf16),
            vmem((n2, n1), bf16),
            vmem((1, n1), f32),
            vmem(packet, f32),
            vmem(packet, f32),
            vmem((plane * cores, width, shard), bf16),
            vmem((plane * cores, STATS, shard), f32),
            vmem((plane * cores, width, shard), bf16),
            vmem((plane * cores, STATS, shard), f32),
            vmem((high, width, shard), bf16),
            vmem((high, STATS, shard), f32),
            vmem((high, width, shard), bf16),
            vmem((high, STATS, shard), f32),
            dma((4,)),
        ]
        + [dma((plane,))] * 8
        + [dma((high,))] * 8
        + [dma((plane * cores,))] * 4,
        compiler_params=pltpu.CompilerParams(
            collective_id=0,
            has_side_effects=True,
        ),
        name="match",
    )(feat_one, feat_two, value_one, value_two)
    return pl.pallas_call(
        place,
        out_shape=(
            jax.ShapeDtypeStruct((shard, width), f32),
            jax.ShapeDtypeStruct((2, shard), f32),
            jax.ShapeDtypeStruct((shard, width), f32),
            jax.ShapeDtypeStruct((2, shard), f32),
        ),
        in_specs=[pl.BlockSpec(memory_space=pltpu.VMEM)] * 2,
        out_specs=[pl.BlockSpec(memory_space=pltpu.VMEM)] * 4,
        name="place",
    )(one, two)


def solution(mesh):
    return jax.shard_map(
        body,
        mesh=mesh,
        in_specs=(
            P(("row", "col"), None),
            P(("col", "row"), None),
            P(("row", "col"), None),
            P(("col", "row"), None),
        ),
        out_specs=(
            P(("row", "col"), None),
            P(None, ("row", "col")),
            P(("col", "row"), None),
            P(None, ("col", "row")),
        ),
        check_vma=False,
    )
```

```python
import functools
import math

import jax
import jax.numpy as jnp
from jax import lax
from jax.experimental import pallas as pl
from jax.experimental.pallas import tpu as pltpu
from jax.sharding import PartitionSpec as P

GRID_W = 256
EXTRA = 16
STATS = 8
SPAN = 240.0
MESH = pl.DeviceIdType.MESH


def split_axes(rows, cols):
    cores = 2 if cols % 2 == 0 else 1
    outer = cols // cores
    low = min(
        (n for n in range(1, rows + 1) if rows % n == 0),
        key=lambda n: abs(n * outer - rows // n),
    )
    return rows // low, low, outer, cores


def coords(block, shard, total, shape):
    index = block * shard + lax.broadcasted_iota(jnp.int32, shape, len(shape) - 1)
    across = lax.rem(index, GRID_W).astype(jnp.float32) / GRID_W
    down = lax.div(index, GRID_W).astype(jnp.float32) / (total // GRID_W)
    return across, down


def values_under(block, value, shard, total):
    across, down = coords(block, shard, total, (EXTRA, shard))
    line = lax.broadcasted_iota(jnp.int32, (EXTRA, shard), 0)
    extra = jnp.where(line == 0, 1.0, jnp.where(line == 1, across, jnp.where(line == 2, down, 0.0)))
    turned = jnp.transpose(value.astype(jnp.float32))
    return jnp.concatenate([turned, extra], axis=0).astype(jnp.bfloat16)


def weigh(keys, queries, rate):
    scores = lax.dot_general(
        keys, queries, (((1,), (1,)), ((), ())), preferred_element_type=jnp.float32
    )
    peak = jnp.max(scores, axis=0, keepdims=True)
    return jnp.exp2((scores - peak) * rate).astype(jnp.bfloat16), peak


def collect(under, weight, peak, width):
    sums = jnp.dot(under, weight, preferred_element_type=jnp.float32)
    acc, stats = sums[:width], sums[width : width + STATS]
    line = lax.broadcasted_iota(jnp.int32, stats.shape, 0)
    return acc, jnp.where(line == 3, peak, stats)


def encode(acc, stats):
    size = jnp.abs(acc)
    big = jnp.maximum(jnp.max(size, axis=0, keepdims=True), 1e-30)
    code = jnp.exp2(size * (SPAN / big) - SPAN / 2)
    line = lax.broadcasted_iota(jnp.int32, stats.shape, 0)
    return jnp.where(acc < 0, -code, code).astype(jnp.bfloat16), jnp.where(line == 4, big, stats)


def decode(code, stats):
    code = code.astype(jnp.float32)
    size = jnp.log(jnp.abs(code)) * (1.0 / (SPAN * math.log(2.0))) + 0.5
    return jnp.where(code < 0, -size, size) * stats[4:5]


def merge(packets, rate):
    top = functools.reduce(jnp.maximum, [stats[3:4] for _, stats in packets])
    acc_all, stats_all = 0.0, 0.0
    for acc, stats in packets:
        factor = jnp.exp2((stats[3:4] - top) * rate)
        acc_all += acc * factor
        stats_all += stats * factor
    return acc_all, stats_all


def kernel(
    dims, total, rate,
    feat_one, feat_two, value_one, value_two,
    out_one, out_two,
    f1, v1, f2, v2, under1, under2, weight1, peak1, weight2, peak2, own1, own2,
    code1, stat1, got_code1, got_stat1, code2, stat2, got_code2, got_stat2,
    load_sem, f1s, f1r, v1s, v1r, g1s, g1r, w1s, w1r, f2s, f2r, v2s, v2r,
    c2s, c2r, t2s, t2r, c1s, c1r, t1s, t1r,
):
    high, low, outer, cores = dims
    rows, cols = high * low, outer * cores
    plane = low * outer
    shard, width = feat_one.shape
    row, col = lax.axis_index("row"), lax.axis_index("col")
    h, l = row // low, row % low
    x, k = col // cores, col % cores
    p = l * outer + x

    def in_plane(step, kind=0):
        q = (p + step + plane) % plane
        return (h * low + q // outer, (q % outer) * cores + (cores - 1 - k if kind else k))

    def in_line(step):
        return (((h + step + high) % high) * low + l, col)

    partner = in_plane(0, 1)

    def block_one(slot):
        q = (p - slot % plane + plane) % plane
        core = k if slot < plane else cores - 1 - k
        return (h * low + q // outer) * cols + (q % outer) * cores + core

    def block_two(slot):
        return col * rows + ((h - slot + high) % high) * low + l

    def span(slot):
        return pl.ds(slot * shard, shard)

    loads = [
        pltpu.make_async_copy(src, dst.at[span(0)], load_sem.at[n])
        for n, (src, dst) in enumerate(
            ((feat_two, f2), (feat_one, f1), (value_one, v1), (value_two, v2))
        )
    ]
    for load in loads:
        load.start()

    peers = [in_line(e) for e in range(1, high)]
    peers += [in_plane(d, kind) for kind in range(cores) for d in range(plane) if d or kind]
    barrier = pltpu.get_barrier_semaphore()
    for peer in peers:
        pl.semaphore_signal(barrier, inc=1, device_id=peer, device_id_type=MESH)
    pl.semaphore_wait(barrier, len(peers))

    started = []

    def send(src, dst, ssem, rsem, peer):
        copy = pltpu.make_async_remote_copy(
            src_ref=src, dst_ref=dst, send_sem=ssem, recv_sem=rsem,
            device_id=peer, device_id_type=MESH,
        )
        copy.start()
        started.append(copy)
        return copy

    def gather(buf, ssem, rsem, count, peer_of):
        return [None] + [
            send(buf.at[span(0)], buf.at[span(s)], ssem.at[s], rsem.at[s], peer_of(s))
            for s in range(1, count)
        ]

    def forward(buf, slot, ssem, rsem):
        return send(
            buf.at[span(slot)], buf.at[span(plane + slot)], ssem.at[slot], rsem.at[slot], partner
        )

    loads[0].wait()
    f2c = gather(f2, f2s, f2r, high, in_line)
    loads[1].wait()
    f1c = gather(f1, f1s, f1r, plane, in_plane)
    loads[2].wait()
    v1c = gather(v1, v1s, v1r, plane, in_plane)
    loads[3].wait()
    v2c = gather(v2, v2s, v2r, high, in_line)
    f1f, v1f = [], []

    def keep_one(slot):
        under1[:, span(slot)] = values_under(block_one(slot), v1[span(slot), :], shard, total)

    for s in range(plane):
        if s:
            f1c[s].wait_recv()
        if cores == 2:
            f1f.append(forward(f1, s, g1s, g1r))
    for s in range(plane):
        if s:
            v1c[s].wait_recv()
        if cores == 2:
            v1f.append(forward(v1, s, w1s, w1r))
        keep_one(s)
    for copy in f1f:
        copy.wait_recv()

    c2c, c1c = {}, {}
    step = 2 if plane % 2 == 0 else 1
    wide = 2 if high % 2 == 0 else 1
    for s in range(high):
        if s:
            f2c[s].wait_recv()
        if s % wide == wide - 1:
            at = pl.ds((s - wide + 1) * shard, wide * shard)
            weight2[:, at], peak2[:, at] = weigh(f1[...], f2[at, :], rate)
    for s, copy in enumerate(v1f):
        copy.wait_recv()
        keep_one(plane + s)
    for s in reversed(range(0, high, wide)):
        at = pl.ds(s * shard, wide * shard)
        accs, statss = collect(under1[...], weight2[:, at], peak2[:, at], width)
        for n in range(wide):
            slot, lanes = s + n, slice(n * shard, (n + 1) * shard)
            acc, stats = accs[:, lanes], statss[:, lanes]
            if slot:
                back = in_line(-slot)
                code2[slot], stat2[slot] = encode(acc, stats)
                c2c[slot] = (
                    send(code2.at[slot], got_code2.at[slot], c2s.at[slot], c2r.at[slot], back),
                    send(stat2.at[slot], got_stat2.at[slot], t2s.at[slot], t2r.at[slot], back),
                )
            else:
                own2[:width], own2[width:] = acc, stats
    for s in reversed(range(0, plane * cores, step)):
        at = pl.ds(s * shard, step * shard)
        weight1[:, at], peak1[:, at] = weigh(f2[...], f1[at, :], rate)
    for s in range(high):
        if s:
            v2c[s].wait_recv()
        under2[:, span(s)] = values_under(block_two(s), v2[span(s), :], shard, total)
    order = sorted(range(0, plane * cores, step), key=lambda s: (-(s % plane), s))
    for s in order:
        at = pl.ds(s * shard, step * shard)
        accs, statss = collect(under2[...], weight1[:, at], peak1[:, at], width)
        for n in range(step):
            slot, lanes = s + n, slice(n * shard, (n + 1) * shard)
            acc, stats = accs[:, lanes], statss[:, lanes]
            if slot:
                owner = in_plane(-(slot % plane), slot // plane)
                code1[slot], stat1[slot] = encode(acc, stats)
                c1c[slot] = (
                    send(code1.at[slot], got_code1.at[slot], c1s.at[slot], c1r.at[slot], owner),
                    send(stat1.at[slot], got_stat1.at[slot], t1s.at[slot], t1r.at[slot], owner),
                )
            else:
                own1[:width], own1[width:] = acc, stats

    def finish(own, copies, codes, stats, block, out):
        packets = [(own[:width], own[width:])]
        for slot, pair in copies.items():
            for copy in pair:
                copy.wait_recv()
            packets.append((decode(codes[slot], stats[slot]), stats[slot]))
        acc, sums = merge(packets, rate)
        inverse = 1.0 / sums[0:1]
        out[:width] = acc * inverse
        across, down = coords(block, shard, total, (STATS, shard))
        line = lax.broadcasted_iota(jnp.int32, sums.shape, 0)
        out[width:] = sums * inverse - jnp.where(line == 1, across, down)

    finish(own2, c2c, got_code2, got_stat2, block_two(0), out_two)
    finish(own1, c1c, got_code1, got_stat1, block_one(0), out_one)
    for copy in started:
        copy.wait_send()


def place(one, two, matched_one, flow_one, matched_two, flow_two):
    width = matched_one.shape[1]
    for packet, matched, flow in ((one, matched_one, flow_one), (two, matched_two, flow_two)):
        matched[...] = jnp.transpose(packet[:width])
        flow[...] = packet[width + 1 : width + 3]


def body(feat_one, feat_two, value_one, value_two):
    shard, width = feat_one.shape
    rows, cols = lax.axis_size("row"), lax.axis_size("col")
    dims = split_axes(rows, cols)
    high, low, outer, cores = dims
    plane = low * outer
    total = shard * rows * cols
    rate = math.log2(math.e) / math.sqrt(width)
    bf16, f32 = jnp.bfloat16, jnp.float32
    n1, n2 = plane * cores * shard, high * shard
    packet = (width + STATS, shard)
    vmem = pltpu.VMEM
    dma = pltpu.SemaphoreType.DMA
    one, two = pl.pallas_call(
        functools.partial(kernel, dims, total, rate),
        out_shape=(pltpu.VMEM(packet, f32),) * 2,
        in_specs=[pl.BlockSpec(memory_space=pltpu.HBM)] * 4,
        out_specs=[pl.BlockSpec(memory_space=pltpu.VMEM)] * 2,
        scratch_shapes=[
            vmem((n1, width), bf16),
            vmem((n1, width), bf16),
            vmem((n2, width), bf16),
            vmem((n2, width), bf16),
            vmem((width + EXTRA, n1), bf16),
            vmem((width + EXTRA, n2), bf16),
            vmem((n2, n1), bf16),
            vmem((1, n1), f32),
            vmem((n1, n2), bf16),
            vmem((1, n2), f32),
            vmem(packet, f32),
            vmem(packet, f32),
            vmem((plane * cores, width, shard), bf16),
            vmem((plane * cores, STATS, shard), f32),
            vmem((plane * cores, width, shard), bf16),
            vmem((plane * cores, STATS, shard), f32),
            vmem((high, width, shard), bf16),
            vmem((high, STATS, shard), f32),
            vmem((high, width, shard), bf16),
            vmem((high, STATS, shard), f32),
            dma((4,)),
        ]
        + [dma((plane,))] * 8
        + [dma((high,))] * 8
        + [dma((plane * cores,))] * 4,
        compiler_params=pltpu.CompilerParams(
            collective_id=0,
            has_side_effects=True,
        ),
        name="match",
    )(feat_one, feat_two, value_one, value_two)
    return pl.pallas_call(
        place,
        out_shape=(
            jax.ShapeDtypeStruct((shard, width), f32),
            jax.ShapeDtypeStruct((2, shard), f32),
            jax.ShapeDtypeStruct((shard, width), f32),
            jax.ShapeDtypeStruct((2, shard), f32),
        ),
        in_specs=[pl.BlockSpec(memory_space=pltpu.VMEM)] * 2,
        out_specs=[pl.BlockSpec(memory_space=pltpu.VMEM)] * 4,
        compiler_params=pltpu.CompilerParams(vmem_limit_bytes=8 << 20),
        name="place",
    )(one, two)


def solution(mesh):
    return jax.shard_map(
        body,
        mesh=mesh,
        in_specs=(
            P(("row", "col"), None),
            P(("col", "row"), None),
            P(("row", "col"), None),
            P(("col", "row"), None),
        ),
        out_specs=(
            P(("row", "col"), None),
            P(None, ("row", "col")),
            P(("col", "row"), None),
            P(None, ("col", "row")),
        ),
        check_vma=False,
    )
```

```python
import functools
import math

import jax
import jax.numpy as jnp
from jax import lax
from jax.experimental import pallas as pl
from jax.experimental.pallas import tpu as pltpu
from jax.sharding import PartitionSpec as P

GRID_W = 256
EXTRA = 16
STATS = 8
SPAN = 240.0
MESH = pl.DeviceIdType.MESH


def split_axes(rows, cols):
    cores = 2 if cols % 2 == 0 else 1
    outer = cols // cores
    low = min(
        (n for n in range(1, rows + 1) if rows % n == 0),
        key=lambda n: abs(n * outer - rows // n),
    )
    return rows // low, low, outer, cores


def coords(block, shard, total, shape):
    index = block * shard + lax.broadcasted_iota(jnp.int32, shape, len(shape) - 1)
    across = lax.rem(index, GRID_W).astype(jnp.float32) / GRID_W
    down = lax.div(index, GRID_W).astype(jnp.float32) / (total // GRID_W)
    return across, down


def values_under(block, value, shard, total):
    across, down = coords(block, shard, total, (EXTRA, shard))
    line = lax.broadcasted_iota(jnp.int32, (EXTRA, shard), 0)
    extra = jnp.where(line == 0, 1.0, jnp.where(line == 1, across, jnp.where(line == 2, down, 0.0)))
    turned = jnp.transpose(value.astype(jnp.float32))
    return jnp.concatenate([turned, extra], axis=0).astype(jnp.bfloat16)


def weigh(keys, queries, rate):
    scores = lax.dot_general(
        keys, queries, (((1,), (1,)), ((), ())), preferred_element_type=jnp.float32
    )
    peak = jnp.max(scores, axis=0, keepdims=True)
    return jnp.exp2((scores - peak) * rate).astype(jnp.bfloat16), peak


def collect(under, weight, peak, width):
    sums = jnp.dot(under, weight, preferred_element_type=jnp.float32)
    acc, stats = sums[:width], sums[width : width + STATS]
    line = lax.broadcasted_iota(jnp.int32, stats.shape, 0)
    return acc, jnp.where(line == 3, peak, stats)


def encode(acc, stats):
    size = jnp.abs(acc)
    big = jnp.maximum(jnp.max(size, axis=0, keepdims=True), 1e-30)
    code = jnp.exp2(size * (SPAN / big) - SPAN / 2)
    line = lax.broadcasted_iota(jnp.int32, stats.shape, 0)
    return jnp.where(acc < 0, -code, code).astype(jnp.bfloat16), jnp.where(line == 4, big, stats)


def decode(code, stats):
    code = code.astype(jnp.float32)
    size = jnp.log(jnp.abs(code)) * (1.0 / (SPAN * math.log(2.0))) + 0.5
    return jnp.where(code < 0, -size, size) * stats[4:5]


def merge(packets, rate):
    top = functools.reduce(jnp.maximum, [stats[3:4] for _, stats in packets])
    acc_all, stats_all = 0.0, 0.0
    for acc, stats in packets:
        factor = jnp.exp2((stats[3:4] - top) * rate)
        acc_all += acc * factor
        stats_all += stats * factor
    return acc_all, stats_all


def kernel(
    dims, total, rate,
    feat_one, feat_two, value_one, value_two,
    out_one, out_two,
    f1, v1, f2, v2, under1, under2, weight1, peak1, weight2, peak2, own1, own2,
    code1, stat1, got_code1, got_stat1, code2, stat2, got_code2, got_stat2,
    load_sem, f1s, f1r, v1s, v1r, g1s, g1r, w1s, w1r, f2s, f2r, v2s, v2r,
    c2s, c2r, t2s, t2r, c1s, c1r, t1s, t1r,
):
    high, low, outer, cores = dims
    rows, cols = high * low, outer * cores
    plane = low * outer
    shard, width = feat_one.shape
    row, col = lax.axis_index("row"), lax.axis_index("col")
    h, l = row // low, row % low
    x, k = col // cores, col % cores
    p = l * outer + x

    def in_plane(step, kind=0):
        q = (p + step + plane) % plane
        return (h * low + q // outer, (q % outer) * cores + (cores - 1 - k if kind else k))

    def in_line(step):
        return (((h + step + high) % high) * low + l, col)

    partner = in_plane(0, 1)

    def block_one(slot):
        q = (p - slot % plane + plane) % plane
        core = k if slot < plane else cores - 1 - k
        return (h * low + q // outer) * cols + (q % outer) * cores + core

    def block_two(slot):
        return col * rows + ((h - slot + high) % high) * low + l

    def span(slot):
        return pl.ds(slot * shard, shard)

    loads = [
        pltpu.make_async_copy(src, dst.at[span(0)], load_sem.at[n])
        for n, (src, dst) in enumerate(
            ((feat_two, f2), (feat_one, f1), (value_one, v1), (value_two, v2))
        )
    ]
    for load in loads:
        load.start()

    peers = [in_line(e) for e in range(1, high)]
    peers += [in_plane(d, kind) for kind in range(cores) for d in range(plane) if d or kind]
    barrier = pltpu.get_barrier_semaphore()
    for peer in peers:
        pl.semaphore_signal(barrier, inc=1, device_id=peer, device_id_type=MESH)
    pl.semaphore_wait(barrier, len(peers))

    started = []

    def send(src, dst, ssem, rsem, peer):
        copy = pltpu.make_async_remote_copy(
            src_ref=src, dst_ref=dst, send_sem=ssem, recv_sem=rsem,
            device_id=peer, device_id_type=MESH,
        )
        copy.start()
        started.append(copy)
        return copy

    def gather(buf, ssem, rsem, count, peer_of):
        return [None] + [
            send(buf.at[span(0)], buf.at[span(s)], ssem.at[s], rsem.at[s], peer_of(s))
            for s in range(1, count)
        ]

    def forward(buf, slot, ssem, rsem):
        return send(
            buf.at[span(slot)], buf.at[span(plane + slot)], ssem.at[slot], rsem.at[slot], partner
        )

    loads[0].wait()
    f2c = gather(f2, f2s, f2r, high, in_line)
    loads[1].wait()
    f1c = gather(f1, f1s, f1r, plane, in_plane)
    loads[2].wait()
    v1c = gather(v1, v1s, v1r, plane, in_plane)
    loads[3].wait()
    v2c = gather(v2, v2s, v2r, high, in_line)
    f1f, v1f = [], []

    def keep_one(slot):
        under1[:, span(slot)] = values_under(block_one(slot), v1[span(slot), :], shard, total)

    for s in range(plane):
        if s:
            f1c[s].wait_recv()
        if cores == 2:
            f1f.append(forward(f1, s, g1s, g1r))
    for s in range(plane):
        if s:
            v1c[s].wait_recv()
        if cores == 2:
            v1f.append(forward(v1, s, w1s, w1r))
        keep_one(s)
    for copy in f1f:
        copy.wait_recv()

    c2c, c1c = {}, {}
    step = 2 if plane % 2 == 0 else 1
    wide = 2 if high % 2 == 0 else 1
    for s in range(high):
        if s:
            f2c[s].wait_recv()
        if s % wide == wide - 1:
            at = pl.ds((s - wide + 1) * shard, wide * shard)
            weight2[:, at], peak2[:, at] = weigh(f1[...], f2[at, :], rate)
    for s in reversed(range(0, plane * cores, step)):
        at = pl.ds(s * shard, step * shard)
        weight1[:, at], peak1[:, at] = weigh(f2[...], f1[at, :], rate)
    for s, copy in enumerate(v1f):
        copy.wait_recv()
        keep_one(plane + s)
    for s in reversed(range(0, high, wide)):
        at = pl.ds(s * shard, wide * shard)
        accs, statss = collect(under1[...], weight2[:, at], peak2[:, at], width)
        for n in range(wide):
            slot, lanes = s + n, slice(n * shard, (n + 1) * shard)
            acc, stats = accs[:, lanes], statss[:, lanes]
            if slot:
                back = in_line(-slot)
                code2[slot], stat2[slot] = encode(acc, stats)
                c2c[slot] = (
                    send(code2.at[slot], got_code2.at[slot], c2s.at[slot], c2r.at[slot], back),
                    send(stat2.at[slot], got_stat2.at[slot], t2s.at[slot], t2r.at[slot], back),
                )
            else:
                own2[:width], own2[width:] = acc, stats
    for s in range(high):
        if s:
            v2c[s].wait_recv()
        under2[:, span(s)] = values_under(block_two(s), v2[span(s), :], shard, total)
    order = sorted(range(0, plane * cores, step), key=lambda s: (-(s % plane), s))
    for s in order:
        at = pl.ds(s * shard, step * shard)
        accs, statss = collect(under2[...], weight1[:, at], peak1[:, at], width)
        for n in range(step):
            slot, lanes = s + n, slice(n * shard, (n + 1) * shard)
            acc, stats = accs[:, lanes], statss[:, lanes]
            if slot:
                owner = in_plane(-(slot % plane), slot // plane)
                code1[slot], stat1[slot] = encode(acc, stats)
                c1c[slot] = (
                    send(code1.at[slot], got_code1.at[slot], c1s.at[slot], c1r.at[slot], owner),
                    send(stat1.at[slot], got_stat1.at[slot], t1s.at[slot], t1r.at[slot], owner),
                )
            else:
                own1[:width], own1[width:] = acc, stats

    def finish(own, copies, codes, stats, block, out):
        packets = [(own[:width], own[width:])]
        for slot, pair in copies.items():
            for copy in pair:
                copy.wait_recv()
            packets.append((decode(codes[slot], stats[slot]), stats[slot]))
        acc, sums = merge(packets, rate)
        inverse = 1.0 / sums[0:1]
        out[:width] = acc * inverse
        across, down = coords(block, shard, total, (STATS, shard))
        line = lax.broadcasted_iota(jnp.int32, sums.shape, 0)
        out[width:] = sums * inverse - jnp.where(line == 1, across, down)

    finish(own2, c2c, got_code2, got_stat2, block_two(0), out_two)
    finish(own1, c1c, got_code1, got_stat1, block_one(0), out_one)
    for copy in started:
        copy.wait_send()


def place(one, two, matched_one, flow_one, matched_two, flow_two):
    width = matched_one.shape[1]
    for packet, matched, flow in ((one, matched_one, flow_one), (two, matched_two, flow_two)):
        matched[...] = jnp.transpose(packet[:width])
        flow[...] = packet[width + 1 : width + 3]


def body(feat_one, feat_two, value_one, value_two):
    shard, width = feat_one.shape
    rows, cols = lax.axis_size("row"), lax.axis_size("col")
    dims = split_axes(rows, cols)
    high, low, outer, cores = dims
    plane = low * outer
    total = shard * rows * cols
    rate = math.log2(math.e) / math.sqrt(width)
    bf16, f32 = jnp.bfloat16, jnp.float32
    n1, n2 = plane * cores * shard, high * shard
    packet = (width + STATS, shard)
    vmem = pltpu.VMEM
    dma = pltpu.SemaphoreType.DMA
    one, two = pl.pallas_call(
        functools.partial(kernel, dims, total, rate),
        out_shape=(pltpu.VMEM(packet, f32),) * 2,
        in_specs=[pl.BlockSpec(memory_space=pltpu.HBM)] * 4,
        out_specs=[pl.BlockSpec(memory_space=pltpu.VMEM)] * 2,
        scratch_shapes=[
            vmem((n1, width), bf16),
            vmem((n1, width), bf16),
            vmem((n2, width), bf16),
            vmem((n2, width), bf16),
            vmem((width + EXTRA, n1), bf16),
            vmem((width + EXTRA, n2), bf16),
            vmem((n2, n1), bf16),
            vmem((1, n1), f32),
            vmem((n1, n2), bf16),
            vmem((1, n2), f32),
            vmem(packet, f32),
            vmem(packet, f32),
            vmem((plane * cores, width, shard), bf16),
            vmem((plane * cores, STATS, shard), f32),
            vmem((plane * cores, width, shard), bf16),
            vmem((plane * cores, STATS, shard), f32),
            vmem((high, width, shard), bf16),
            vmem((high, STATS, shard), f32),
            vmem((high, width, shard), bf16),
            vmem((high, STATS, shard), f32),
            dma((4,)),
        ]
        + [dma((plane,))] * 8
        + [dma((high,))] * 8
        + [dma((plane * cores,))] * 4,
        compiler_params=pltpu.CompilerParams(
            collective_id=0,
            has_side_effects=True,
        ),
        name="match",
    )(feat_one, feat_two, value_one, value_two)
    return pl.pallas_call(
        place,
        out_shape=(
            jax.ShapeDtypeStruct((shard, width), f32),
            jax.ShapeDtypeStruct((2, shard), f32),
            jax.ShapeDtypeStruct((shard, width), f32),
            jax.ShapeDtypeStruct((2, shard), f32),
        ),
        in_specs=[pl.BlockSpec(memory_space=pltpu.VMEM)] * 2,
        out_specs=[pl.BlockSpec(memory_space=pltpu.VMEM)] * 4,
        compiler_params=pltpu.CompilerParams(vmem_limit_bytes=8 << 20),
        name="place",
    )(one, two)


def solution(mesh):
    return jax.shard_map(
        body,
        mesh=mesh,
        in_specs=(
            P(("row", "col"), None),
            P(("col", "row"), None),
            P(("row", "col"), None),
            P(("col", "row"), None),
        ),
        out_specs=(
            P(("row", "col"), None),
            P(None, ("row", "col")),
            P(("col", "row"), None),
            P(None, ("col", "row")),
        ),
        check_vma=False,
    )
```
